32 devices in a mesh: data: 1 (over z), model: 4 (over y), stage: 8 (over x, core).
Axes of the slice: x: 4, y: 4, z: 1, core: 2. Of those that a mesh axis runs over, the one named last changes fastest.
The devices are a block of a 4x4x8 slice.
Arguments:
- inputs: bfloat16 [8, 256, 1536], P('data')
- targets: bfloat16 [8, 256, 1536], P('data')
- w_in: bfloat16 [8, 1, 1536, 6144], P('stage', None, None, 'model')
- w_out: bfloat16 [8, 1, 6144, 1536], P('stage', None, 'model')
Outputs:
- output 1: float32 [8, 1, 1536, 6144], P(('data', 'stage'), None, None, 'model')
- output 2: float32 [8, 1, 6144, 1536], P(('data', 'stage'), None, 'model')
- output 3: float32 [1], P('data')
All inputs are finite; a program needn't handle non-finite values.
Results may differ from the reference program's by a relative error of at most 0.00704361.
Values are sent between devices in bfloat16 or wider.
A program may use at most 768 MiB of HBM per device.

```python
import jax
import jax.numpy as jnp
from jax import lax

STAGES = 8
LAYERS_PER_STAGE = 1
MODEL_DIM = 1536
HIDDEN_DIM = 6144
MICRO_BATCHES = 8
MICRO_TOKENS = 256

TOTAL_LAYERS = STAGES * LAYERS_PER_STAGE
GELU_COEF = 0.7978845608028654
CUBIC_COEF = 0.044715


def gelu_tanh(values):
    inner_arg = GELU_COEF * (values + CUBIC_COEF * values * values * values)
    return 0.5 * values * (1.0 + jnp.tanh(inner_arg))


def gelu_slope(values):
    tanh_val = jnp.tanh(GELU_COEF * (values + CUBIC_COEF * values * values * values))
    return 0.5 * (1.0 + tanh_val) + 0.5 * values * (1.0 - tanh_val * tanh_val) * GELU_COEF * (1.0 + 3.0 * CUBIC_COEF * values * values)


def setup_inputs(seed: int = 0, part: int = 0) -> dict:
    part_key = jax.random.fold_in(jax.random.key(seed), part)
    key_in, key_tgt = jax.random.split(part_key, 2)
    key_w1, key_w2 = jax.random.split(jax.random.key(seed + 1), 2)
    act_shape = (MICRO_BATCHES, MICRO_TOKENS, MODEL_DIM)
    inputs = jax.random.normal(key_in, act_shape, jnp.float32).astype(jnp.bfloat16)
    targets = jax.random.normal(key_tgt, act_shape, jnp.float32).astype(jnp.bfloat16)
    in_scale = MODEL_DIM ** -0.5
    out_scale = (HIDDEN_DIM ** -0.5) * (2.0 / TOTAL_LAYERS) ** 0.5
    w_in = (jax.random.normal(key_w1, (STAGES, LAYERS_PER_STAGE, MODEL_DIM, HIDDEN_DIM), jnp.float32) * in_scale).astype(jnp.bfloat16)
    w_out = (jax.random.normal(key_w2, (STAGES, LAYERS_PER_STAGE, HIDDEN_DIM, MODEL_DIM), jnp.float32) * out_scale).astype(jnp.bfloat16)
    return {"inputs": inputs, "targets": targets, "w_in": w_in, "w_out": w_out}


def layer_forward(hidden, w_in_l, w_out_l):
    pre_act = jnp.dot(hidden, w_in_l, preferred_element_type=jnp.float32).astype(jnp.bfloat16)
    act_out = gelu_tanh(pre_act.astype(jnp.float32)).astype(jnp.bfloat16)
    branch = jnp.dot(act_out, w_out_l, preferred_element_type=jnp.float32)
    return (hidden.astype(jnp.float32) + branch).astype(jnp.bfloat16)


def layer_backward(grad_h, hidden, w_in_l, w_out_l):
    pre_act = jnp.dot(hidden, w_in_l, preferred_element_type=jnp.float32).astype(jnp.bfloat16)
    act_out = gelu_tanh(pre_act.astype(jnp.float32)).astype(jnp.bfloat16)
    grad_act = jnp.dot(grad_h, w_out_l.T, preferred_element_type=jnp.float32).astype(jnp.bfloat16)
    grad_pre = (gelu_slope(pre_act.astype(jnp.float32)) * grad_act.astype(jnp.float32)).astype(jnp.bfloat16)
    grad_prev = (grad_h.astype(jnp.float32) + jnp.dot(grad_pre, w_in_l.T, preferred_element_type=jnp.float32)).astype(jnp.bfloat16)
    part_in = jnp.dot(hidden.T, grad_pre, preferred_element_type=jnp.float32)
    part_out = jnp.dot(act_out.T, grad_h, preferred_element_type=jnp.float32)
    return grad_prev, part_in, part_out


def reference(inputs, targets, w_in, w_out):
    w_in_flat = w_in.reshape(TOTAL_LAYERS, MODEL_DIM, HIDDEN_DIM)
    w_out_flat = w_out.reshape(TOTAL_LAYERS, HIDDEN_DIM, MODEL_DIM)
    grad_scale = 1.0 / (MICRO_BATCHES * MICRO_TOKENS * MODEL_DIM)

    def fwd_step(hidden, layer_w):
        return layer_forward(hidden, layer_w[0], layer_w[1]), hidden

    def bwd_step(grad_h, layer_data):
        w_in_l, w_out_l, saved_in, acc_in, acc_out = layer_data
        grad_prev, part_in, part_out = layer_backward(grad_h, saved_in, w_in_l, w_out_l)
        return grad_prev, (acc_in + part_in, acc_out + part_out)

    def micro_step(state_in, micro_pair):
        acc_in, acc_out, loss_sum = state_in
        final_out, saved_in = lax.scan(fwd_step, micro_pair[0], (w_in_flat, w_out_flat))
        out_err = final_out.astype(jnp.float32) - micro_pair[1].astype(jnp.float32)
        start_grad = (out_err * grad_scale).astype(jnp.bfloat16)
        input_grad, (acc_in, acc_out) = lax.scan(bwd_step, start_grad, (w_in_flat, w_out_flat, saved_in, acc_in, acc_out), reverse=True)
        return (acc_in, acc_out, loss_sum + 0.5 * jnp.sum(out_err * out_err)), None

    init_state = (jnp.zeros((TOTAL_LAYERS, MODEL_DIM, HIDDEN_DIM), jnp.float32), jnp.zeros((TOTAL_LAYERS, HIDDEN_DIM, MODEL_DIM), jnp.float32), jnp.zeros((), jnp.float32))
    (acc_in, acc_out, loss_sum), unused_ys = lax.scan(micro_step, init_state, (inputs, targets))
    grad_in = acc_in.reshape(STAGES, LAYERS_PER_STAGE, MODEL_DIM, HIDDEN_DIM)
    grad_out = acc_out.reshape(STAGES, LAYERS_PER_STAGE, HIDDEN_DIM, MODEL_DIM)
    return grad_in, grad_out, jnp.reshape(loss_sum * grad_scale, (1,))
```

```python
import functools

import jax
import jax.numpy as jnp
from jax import lax
from jax.experimental import pallas as pl
from jax.experimental.pallas import tpu as pltpu
from jax.sharding import PartitionSpec as P

GELU_COEF = 0.7978845608028654
CUBIC_COEF = 0.044715
MESH = pl.DeviceIdType.MESH
F32 = jnp.float32
BF16 = jnp.bfloat16

TOKENS = 128
SLOTS = 4
NT = (((1,), (1,)), ((), ()))
TN = (((0,), (0,)), ((), ()))


def dot(a, b, dims=(((1,), (0,)), ((), ()))):
    return lax.dot_general(a, b, dims, preferred_element_type=F32)


def kernel(n_stage, x_hbm, t_hbm, w1_hbm, w2_hbm, dw1_hbm, dw2_hbm, loss_ref,
           w1, w2, dw1, dw2, xs, us, es, ab, gb, ps, rs, outs, tgt, err_acc, ltile,
           load_sem, x_sem, e_sem, r_sem, p_sem, o_sem, l_sem, chain_sem, store_sem):
    n_model = 4
    num, _, rows, width = xs.shape
    tokens = n_model * rows
    hidden = w1.shape[1]
    half = width // 2
    tile = min(512, hidden)
    scale = 1.0 / (num * tokens * width)
    s = lax.axis_index("stage")
    d = lax.axis_index("model")
    right = lax.rem(d + 1, n_model)
    left = lax.rem(d + 3, n_model)
    far = lax.rem(d + 2, n_model)
    first = s == 0
    last = s == n_stage - 1
    up = lax.rem(s + 1, n_stage)
    down = lax.rem(s + n_stage - 1, n_stage)

    def peer(k):
        return lax.rem(d + k, n_model)

    def send(src, dst, ssem, rsem, model, stage):
        return pltpu.make_async_remote_copy(
            src_ref=src, dst_ref=dst, send_sem=ssem, recv_sem=rsem,
            device_id={"model": model, "stage": stage}, device_id_type=MESH)

    def got(ref, sem):
        send(ref, ref, sem, sem, right, s).wait_recv()

    def sent(ref, sem):
        send(ref, ref, sem, sem, right, s).wait_send()

    load_w1 = pltpu.make_async_copy(w1_hbm, w1, load_sem.at[0])
    load_w2 = pltpu.make_async_copy(w2_hbm, w2, load_sem.at[1])
    load_x = pltpu.make_async_copy(x_hbm, xs, load_sem.at[2])
    load_t = pltpu.make_async_copy(t_hbm.at[:, d], tgt, load_sem.at[3])

    @pl.when(first)
    def _():
        load_x.start()

    load_w1.start()
    load_w2.start()

    @pl.when(last)
    def _():
        load_t.start()

    barrier = pltpu.get_barrier_semaphore()
    for k in range(1, n_model):
        pl.semaphore_signal(barrier, inc=1, device_id={"model": peer(k), "stage": s}, device_id_type=MESH)
    for k in range(n_model):
        pl.semaphore_signal(barrier, inc=1, device_id={"model": peer(k), "stage": up}, device_id_type=MESH)
        pl.semaphore_signal(barrier, inc=1, device_id={"model": peer(k), "stage": down}, device_id_type=MESH)

    def zero(i, c):
        r = pl.ds(pl.multiple_of(i * 64, 64), 64)
        dw1[r, :] = jnp.zeros((64, dw1.shape[1]), F32)
        return c

    lax.fori_loop(0, dw1.shape[0] // 64, zero, 0)

    def zero2(i, c):
        r = pl.ds(pl.multiple_of(i * 64, 64), 64)
        dw2[r, :] = jnp.zeros((64, dw2.shape[1]), F32)
        return c

    lax.fori_loop(0, dw2.shape[0] // 64, zero2, 0)
    err_acc[...] = jnp.zeros_like(err_acc)
    pl.semaphore_wait(barrier, 3 * n_model - 1)

    @pl.when(first)
    def _():
        load_x.wait()

    load_w1.wait()
    load_w2.wait()

    @pl.when(last)
    def _():
        load_t.wait()

    def exchange(slot):
        def step(h, o, k, dev):
            return send(ps.at[h, o], rs.at[slot, k], p_sem.at[k], r_sem.at[slot, k], dev, s)

        return (
            step(0, far, 0, right), step(1, far, 1, left),
            step(1, right, 2, right), step(0, left, 3, left),
            step(0, right, 4, right), step(1, left, 5, left),
        )

    def relay_sums(slot):
        ex = exchange(slot)
        got(rs.at[slot, 0], r_sem.at[slot, 0])
        ps[0, right] += rs[slot, 0]
        ex[4].start()
        got(rs.at[slot, 1], r_sem.at[slot, 1])
        ps[1, left] += rs[slot, 1]
        ex[5].start()

    def final_sums(slot, base):
        for k in (2, 3, 4, 5):
            got(rs.at[slot, k], r_sem.at[slot, k])
        h0 = base[:, :half].astype(F32) + (ps[0, d] + rs[slot, 4] + rs[slot, 3])
        h1 = base[:, half:].astype(F32) + (ps[1, d] + rs[slot, 2] + rs[slot, 5])
        return h0.astype(BF16), h1.astype(BF16)

    def sums_sent():
        for k in range(6):
            sent(ps.at[0, 0], p_sem.at[k])

    def fwd(i, c):
        slot = lax.rem(i, SLOTS)

        @pl.when(jnp.logical_not(first))
        def _():
            got(xs.at[i], x_sem.at[i])

        xm = xs[i].reshape(tokens, width)
        for j in range(hidden // tile):
            cols = slice(j * tile, (j + 1) * tile)
            u = dot(xm, w1[:, cols]).astype(BF16)
            us[i, :, cols] = u
            uf = u.astype(F32)
            tau = jnp.tanh(GELU_COEF * (uf + CUBIC_COEF * uf * uf * uf))
            ab[:, cols] = (0.5 * uf * (1.0 + tau)).astype(BF16)
        am = ab[...]
        ex = exchange(slot)
        ps[0] = dot(am, w2[:, :half]).reshape(n_model, rows, half)
        ex[0].start()
        ex[3].start()
        ps[1] = dot(am, w2[:, half:]).reshape(n_model, rows, half)
        ex[1].start()
        ex[2].start()
        relay_sums(slot)
        h0, h1 = final_sums(slot, xs[i, d])

        @pl.when(jnp.logical_not(last))
        def _():
            outs[i, :, :half] = h0
            outs[i, :, half:] = h1
            for k in (2, 1, 3, 0):
                send(outs.at[i], xs.at[i, d], o_sem.at[k], x_sem.at[i], peer(k), up).start()

        @pl.when(last)
        def _():
            for h, v in ((0, h0), (1, h1)):
                cols = slice(h * half, (h + 1) * half)
                err = v.astype(F32) - tgt[i, :, cols].astype(F32)
                es[i, d, :, cols] = (err * scale).astype(BF16)
                err_acc[:, cols] += err * err
            for k in (2, 1, 3):
                send(es.at[i, d], es.at[i, d], o_sem.at[k], e_sem.at[i], peer(k), s).start()

        sums_sent()
        return c

    lax.fori_loop(0, num, fwd, 0)

    for k in (1, 2, 3):
        sent(outs, o_sem.at[k])

    @pl.when(jnp.logical_not(last))
    def _():
        sent(outs, o_sem.at[0])

    def bwd(i, c):
        slot = lax.rem(i, SLOTS)

        @pl.when(last)
        def _():
            got(es.at[i, pl.ds(0, n_model - 1)], e_sem.at[i])

        @pl.when(jnp.logical_not(last))
        def _():
            got(es.at[i], e_sem.at[i])

        em = es[i].reshape(tokens, width)
        for j in range(hidden // tile):
            cols = slice(j * tile, (j + 1) * tile)
            q = dot(em, w2[cols, :], NT).astype(BF16).astype(F32)
            uf = us[i, :, cols].astype(F32)
            sq = uf * uf
            tau = jnp.tanh(GELU_COEF * (uf + CUBIC_COEF * uf * sq))
            slope = 0.5 * (1.0 + tau) + 0.5 * uf * (1.0 - tau * tau) * GELU_COEF * (1.0 + 3.0 * CUBIC_COEF * sq)
            gb[:, cols] = (slope * q).astype(BF16)
            ab[:, cols] = (0.5 * uf * (1.0 + tau)).astype(BF16)

        @pl.when(jnp.logical_not(first))
        def _():
            gm = gb[...]
            ex = exchange(slot)
            ps[0] = dot(gm, w1[:half, :], NT).reshape(n_model, rows, half)
            ex[0].start()
            ex[3].start()
            ps[1] = dot(gm, w1[half:, :], NT).reshape(n_model, rows, half)
            ex[1].start()
            ex[2].start()

        for j in range(hidden // tile):
            r = slice(j * tile, (j + 1) * tile)
            dw2[r, :] += dot(ab[:, r], em, TN)

        @pl.when(jnp.logical_not(first))
        def _():
            relay_sums(slot)

        gm = gb[...]
        for j in range(width // tile):
            r = slice(j * tile, (j + 1) * tile)
            xt = xs[i, :, :, r].reshape(tokens, tile)
            dw1[r, :] += dot(xt, gm, TN)

        @pl.when(jnp.logical_not(first))
        def _():
            h0, h1 = final_sums(slot, es[i, d])
            outs[i, :, :half] = h0
            outs[i, :, half:] = h1
            for k in (2, 1, 3, 0):
                send(outs.at[i], es.at[i, d], o_sem.at[k], e_sem.at[i], peer(k), down).start()
            sums_sent()

        return c

    lax.fori_loop(0, num, bwd, 0)

    store1 = pltpu.make_async_copy(dw1, dw1_hbm, store_sem.at[0])
    store2 = pltpu.make_async_copy(dw2, dw2_hbm, store_sem.at[1])
    store1.start()
    store2.start()

    @pl.when(last)
    def _():
        ltile[d] = jnp.full(ltile.shape[1:], 0.5 * jnp.sum(err_acc[...]), F32)
        for k in (2, 1, 3):
            send(ltile.at[d], ltile.at[d], l_sem.at[k], l_sem.at[n_model], peer(k), s).start()
        got(ltile.at[pl.ds(0, n_model - 1)], l_sem.at[n_model])
        ltile[n_model] = ltile[0] + ltile[1] + ltile[2] + ltile[3]
        for k in (1, 2, 3):
            sent(ltile.at[0], l_sem.at[k])

    @pl.when(jnp.logical_not(last))
    def _():
        got(ltile.at[n_model], chain_sem.at[0])

    @pl.when(jnp.logical_not(first))
    def _():
        chain = send(ltile.at[n_model], ltile.at[n_model], chain_sem.at[1], chain_sem.at[0], d, down)
        chain.start()
        for k in (0, 1, 2, 3):
            sent(outs, o_sem.at[k])
        chain.wait_send()

    loss_ref[...] = ltile[n_model] * scale
    store1.wait()
    store2.wait()


def run_group(n_stage, tokens, x, t, w1, w2):
    num, n_model, rows, width = x.shape
    hidden = w1.shape[1]
    half = width // 2
    any_spec = pl.BlockSpec(memory_space=pl.ANY)
    vmem = pltpu.VMEM
    dma = pltpu.SemaphoreType.DMA
    flops = 12 * num * tokens * width * hidden
    return pl.pallas_call(
        functools.partial(kernel, n_stage),
        out_shape=(
            jax.ShapeDtypeStruct(w1.shape, F32),
            jax.ShapeDtypeStruct(w2.shape, F32),
            jax.ShapeDtypeStruct((8, 128), F32),
        ),
        in_specs=[any_spec] * 4,
        out_specs=(any_spec, any_spec, pl.BlockSpec(memory_space=vmem)),
        scratch_shapes=[
            vmem(w1.shape, BF16),
            vmem(w2.shape, BF16),
            vmem(w1.shape, F32),
            vmem(w2.shape, F32),
            vmem(x.shape, BF16),
            vmem((num, tokens, hidden), BF16),
            vmem(x.shape, BF16),
            vmem((tokens, hidden), BF16),
            vmem((tokens, hidden), BF16),
            vmem((2, n_model, rows, half), F32),
            vmem((SLOTS, 6, rows, half), F32),
            vmem((num, rows, width), BF16),
            vmem((num, rows, width), BF16),
            vmem((rows, width), F32),
            vmem((n_model + 1, 8, 128), F32),
            dma((4,)),
            dma((num,)),
            dma((num,)),
            dma((SLOTS, 6)),
            dma((6,)),
            dma((n_model,)),
            dma((n_model + 1,)),
            dma((2,)),
            dma((2,)),
        ],
        compiler_params=pltpu.CompilerParams(
            collective_id=0, has_side_effects=True, vmem_limit_bytes=67043328
        ),
        cost_estimate=pl.CostEstimate(flops=flops, bytes_accessed=60 * width * hidden // 4, transcendentals=0),
        name="pipeline_step",
    )(x, t, w1, w2)


def solution(mesh):
    n_stage = mesh.shape["stage"]
    n_model = mesh.shape["model"]

    def stage_step(inputs, targets, w_in, w_out):
        width = inputs.shape[-1]
        total = inputs.shape[0] * inputs.shape[1]
        num = total // TOKENS
        shape = (num, n_model, TOKENS // n_model, width)
        dw1, dw2, loss = run_group(
            n_stage, TOKENS, inputs.reshape(shape), targets.reshape(shape), w_in[0, 0], w_out[0, 0])
        return dw1[None, None], dw2[None, None], loss[0, :1]

    return jax.shard_map(
        stage_step,
        mesh=mesh,
        in_specs=(P("data", None, None), P("data", None, None), P("stage", None, None, "model"), P("stage", None, "model", None)),
        out_specs=(P(("data", "stage"), None, None, "model"), P(("data", "stage"), None, "model", None), P("data")),
        check_vma=False,
    )
```

```python
import functools

import jax
import jax.numpy as jnp
from jax import lax
from jax.experimental import pallas as pl
from jax.experimental.pallas import tpu as pltpu
from jax.sharding import PartitionSpec as P

GELU_COEF = 0.7978845608028654
CUBIC_COEF = 0.044715
MESH = pl.DeviceIdType.MESH
F32 = jnp.float32
BF16 = jnp.bfloat16

TOKENS = 64
UNIT = 2
SLOTS = 2 * UNIT
AHEAD = (22, 19, 16, 13, 10, 7, 4, 1)
ORDER = (("A", 0, 0), ("T", 0, 0), ("E5", 1, 1), ("E4", 0, 0), ("A", 1, 0), ("E5", 0, 0), ("G2", 1, 0), ("G1", 1, 0), ("E4", 1, 0))
TN = (((0,), (0,)), ((), ()))


def dot(a, b, dims=(((1,), (0,)), ((), ()))):
    return lax.dot_general(a, b, dims, preferred_element_type=F32)


def kernel(n_stage, x_hbm, t_hbm, w1_hbm, w2_hbm, dw1_hbm, dw2_hbm, loss_ref,
           w1, w2, w1t, w2t, dw1, dw2, xs, us, es, ab, gb, ps, rs, outs, err_acc, ltile,
           load_sem, in_sem, r_sem, p_sem, o_sem, l_sem, chain_sem, store_sem):
    n_model = 4
    num, _, rows, width = xs.shape
    tokens = n_model * rows
    hidden = w1.shape[1]
    half = width // 2
    tile = min(512, hidden)
    scale = 1.0 / (num * tokens * width)
    s = lax.axis_index("stage")
    d = lax.axis_index("model")
    right = lax.rem(d + 1, n_model)
    left = lax.rem(d + 3, n_model)
    far = lax.rem(d + 2, n_model)
    first = s == 0
    last = s == n_stage - 1
    up = lax.rem(s + 1, n_stage)
    down = lax.rem(s + n_stage - 1, n_stage)
    ahead = jnp.int32(0)
    for k in range(n_stage):
        ahead = jnp.where(s == k, AHEAD[len(AHEAD) - n_stage + k], ahead)
    acts = (xs, es)

    def peer(k):
        return lax.rem(d + k, n_model)

    def send(src, dst, ssem, rsem, model, stage):
        return pltpu.make_async_remote_copy(
            src_ref=src, dst_ref=dst, send_sem=ssem, recv_sem=rsem,
            device_id={"model": model, "stage": stage}, device_id_type=MESH)

    def got(ref, sem):
        send(ref, ref, sem, sem, right, s).wait_recv()

    def sent(ref, sem):
        send(ref, ref, sem, sem, right, s).wait_send()

    units = num // UNIT
    tgt = outs.at[0]
    load_w1 = pltpu.make_async_copy(w1_hbm, w1, load_sem.at[0])
    load_w2 = pltpu.make_async_copy(w2_hbm, w2, load_sem.at[1])
    load_x0 = pltpu.make_async_copy(x_hbm.at[pl.ds(0, UNIT)], xs.at[pl.ds(0, UNIT)], load_sem.at[2])
    load_x1 = pltpu.make_async_copy(
        x_hbm.at[pl.ds(UNIT, num - UNIT)], xs.at[pl.ds(UNIT, num - UNIT)], load_sem.at[3])
    load_t = pltpu.make_async_copy(t_hbm.at[:, d], tgt, load_sem.at[4])

    @pl.when(first)
    def _():
        load_x0.start()

    load_w1.start()
    load_w2.start()

    @pl.when(first)
    def _():
        load_x1.start()

    @pl.when(last)
    def _():
        load_t.start()

    barrier = pltpu.get_barrier_semaphore()
    for k in range(1, n_model):
        pl.semaphore_signal(barrier, inc=1, device_id={"model": peer(k), "stage": s}, device_id_type=MESH)
    for k in range(n_model):
        pl.semaphore_signal(barrier, inc=1, device_id={"model": peer(k), "stage": up}, device_id_type=MESH)
        pl.semaphore_signal(barrier, inc=1, device_id={"model": peer(k), "stage": down}, device_id_type=MESH)

    def zero(i, c):
        r = pl.ds(pl.multiple_of(i * 64, 64), 64)
        dw1[r, :] = jnp.zeros((64, dw1.shape[1]), F32)
        return c

    lax.fori_loop(0, dw1.shape[0] // 64, zero, 0)

    def zero2(i, c):
        r = pl.ds(pl.multiple_of(i * 64, 64), 64)
        dw2[r, :] = jnp.zeros((64, dw2.shape[1]), F32)
        return c

    lax.fori_loop(0, dw2.shape[0] // 64, zero2, 0)
    err_acc[...] = jnp.zeros_like(err_acc)
    pl.semaphore_wait(barrier, 3 * n_model - 1)

    pieces = hidden // 128
    assert width == hidden
    lazy = ahead > pieces

    def transpose(c):
        r = pl.ds(pl.multiple_of(c * 128, 128), 128)
        w2t[:, r] = w2[r, :].T
        w1t[:, r] = w1[r, :].T

    @pl.when(jnp.logical_not(lazy))
    def _():
        load_w1.wait()
        load_w2.wait()

        def piece(c, carry):
            transpose(c)
            return carry

        lax.fori_loop(0, pieces, piece, 0)

    @pl.when(last)
    def _():
        load_t.wait()

    def part(f, i, k):
        h, o, dev = ((0, far, right), (1, far, left), (1, right, right), (0, left, left), (0, right, right), (1, left, left))[k]
        b = lax.rem(i, UNIT)
        slot = lax.rem(i, SLOTS)
        return send(ps.at[f, h, b, o], rs.at[f, slot, k], p_sem.at[f, b, k], r_sem.at[f, slot, k], dev, s)

    def sums_sent(f, b):
        for k in range(6):
            sent(ps.at[0, 0, 0, 0], p_sem.at[f, b, k])

    def products(f, u, mat, weight):
        steps = [u * UNIT + k for k in range(UNIT)]

        @pl.when(u >= 1)
        def _():
            for k in range(UNIT):
                sums_sent(f, k)

        for h, kinds in ((0, (0,)), (1, (1, 2, 3))):
            ps[f, h] = weight(mat, h).reshape(UNIT, n_model, rows, half)
            for k in kinds:
                for i in steps:
                    part(f, i, k).start()

    def relay_sums(f, i):
        b = lax.rem(i, UNIT)
        slot = lax.rem(i, SLOTS)
        got(rs.at[f, slot, 0], r_sem.at[f, slot, 0])
        ps[f, 0, b, right] += rs[f, slot, 0]
        part(f, i, 4).start()
        got(rs.at[f, slot, 1], r_sem.at[f, slot, 1])
        ps[f, 1, b, left] += rs[f, slot, 1]
        part(f, i, 5).start()

    def final_sums(f, i):
        b = lax.rem(i, UNIT)
        slot = lax.rem(i, SLOTS)
        for k in (2, 3, 4, 5):
            got(rs.at[f, slot, k], r_sem.at[f, slot, k])
        base = acts[f][i, d]
        h0 = base[:, :half].astype(F32) + (ps[f, 0, b, d] + rs[f, slot, 4] + rs[f, slot, 3])
        h1 = base[:, half:].astype(F32) + (ps[f, 1, b, d] + rs[f, slot, 2] + rs[f, slot, 5])
        return h0.astype(BF16), h1.astype(BF16)

    def spread(f, i, src, stage, sender, here):
        dst = acts[f].at[i, d]
        for k in (2, 1, 3) if here else (2, 1, 3, 0):
            send(src, dst, o_sem.at[sender, k], in_sem.at[f, i], peer(k), stage).start()

    def arrived(f, i):
        if f:
            @pl.when(last)
            def _():
                got(es.at[i, pl.ds(0, n_model - 1)], in_sem.at[f, i])

            @pl.when(jnp.logical_not(last))
            def _():
                got(es.at[i], in_sem.at[f, i])
        else:
            got(xs.at[i], in_sem.at[f, i])

    def unit_rows(ref, u):
        return ref[pl.ds(u * UNIT, UNIT)].reshape(UNIT * tokens, width)

    def fwd(u):
        @pl.when(jnp.logical_not(first))
        def _():
            for k in range(UNIT):
                arrived(0, u * UNIT + k)

        @pl.when(jnp.logical_and(first, u <= 1))
        def _():
            @pl.when(u == 0)
            def _():
                load_x0.wait()

            @pl.when(u == 1)
            def _():
                load_x1.wait()

        start = jnp.logical_and(lazy, u == 0)

        @pl.when(start)
        def _():
            load_w1.wait()

        xm = unit_rows(xs, u)
        for j in range(hidden // tile):
            cols = slice(j * tile, (j + 1) * tile)
            pre = dot(xm, w1[:, cols]).astype(BF16)
            us[u, :, cols] = pre
            uf = pre.astype(F32)
            tau = jnp.tanh(GELU_COEF * (uf + CUBIC_COEF * uf * uf * uf))
            ab[:, cols] = (0.5 * uf * (1.0 + tau)).astype(BF16)

        @pl.when(start)
        def _():
            load_w2.wait()

        products(0, u, ab[...], lambda m, h: dot(m, w2[:, h * half:(h + 1) * half]))

    def fwd_out(i):
        h0, h1 = final_sums(0, i)

        @pl.when(jnp.logical_not(last))
        def _():
            outs[0, i, :, :half] = h0
            outs[0, i, :, half:] = h1
            spread(0, i, outs.at[0, i], up, 0, False)

        @pl.when(last)
        def _():
            for h, v in ((0, h0), (1, h1)):
                cols = slice(h * half, (h + 1) * half)
                err = v.astype(F32) - tgt[i, :, cols].astype(F32)
                es[i, d, :, cols] = (err * scale).astype(BF16)
                err_acc[:, cols] += err * err
            spread(1, i, es.at[i, d], s, 0, True)

    def bwd_out(i):
        h0, h1 = final_sums(1, i)
        outs[1, i, :, :half] = h0
        outs[1, i, :, half:] = h1
        spread(1, i, outs.at[1, i], down, 1, False)

    def saved(which, j):
        src, dst = ((dw1, dw1_hbm), (dw2, dw2_hbm))[which]
        r = pl.ds(j * tile, tile)
        return pltpu.make_async_copy(src.at[r], dst.at[r], store_sem.at[which, j])

    def store(u, which, j):
        @pl.when(u == units - 1)
        def _():
            saved(which, j).start()

    def grad_out(u):
        em = unit_rows(es, u)
        for j in range(hidden // tile):
            r = slice(j * tile, (j + 1) * tile)
            dw2[r, :] += dot(ab[:, r], em, TN)
            store(u, 1, j)

    def grad_in(u):
        gm = gb[...]
        for j in range(width // tile):
            r = slice(j * tile, (j + 1) * tile)
            xt = xs[pl.ds(u * UNIT, UNIT), :, :, r].reshape(UNIT * tokens, tile)
            dw1[r, :] += dot(xt, gm, TN)
            store(u, 0, j)

    def bwd(u):
        for k in range(UNIT):
            arrived(1, u * UNIT + k)
        em = unit_rows(es, u)
        for j in range(hidden // tile):
            cols = slice(j * tile, (j + 1) * tile)
            q = dot(em, w2t[:, cols]).astype(BF16).astype(F32)
            uf = us[u, :, cols].astype(F32)
            sq = uf * uf
            tau = jnp.tanh(GELU_COEF * (uf + CUBIC_COEF * uf * sq))
            slope = 0.5 * (1.0 + tau) + 0.5 * uf * (1.0 - tau * tau) * GELU_COEF * (1.0 + 3.0 * CUBIC_COEF * sq)
            gb[:, cols] = (slope * q).astype(BF16)
            ab[:, cols] = (0.5 * uf * (1.0 + tau)).astype(BF16)

        @pl.when(jnp.logical_not(first))
        def _():
            products(1, u, gb[...], lambda m, h: dot(m, w1t[:, h * half:(h + 1) * half]))

    def op(name, f, lag, tick):
        u = tick - lag - (ahead if f else 0)
        live = jnp.logical_and(u >= 0, u < units)
        if name == "A":
            run = bwd if f else fwd
        elif name == "T":
            run = lambda u: transpose(u - 1)
            live = jnp.logical_and(lazy, jnp.logical_and(u >= 1, u <= pieces))
        elif name == "G2":
            run = grad_out
        elif name == "G1":
            run = grad_in
        else:
            step = {
                "E4": functools.partial(relay_sums, f),
                "E5": bwd_out if f else fwd_out,
            }[name]

            def each(k, c):
                step(u * UNIT + k)
                return c

            def run(u):
                lax.fori_loop(0, UNIT, each, 0)

        if f and name in ("E4", "E5"):
            live = jnp.logical_and(live, jnp.logical_not(first))

        @pl.when(live)
        def _():
            run(u)

    def tick(t, c):
        for name, f, lag in ORDER:
            op(name, f, lag, t)
        return c

    begin = min(lag for _, _, lag in ORDER)
    lax.fori_loop(begin, units + ahead + max(lag for _, f, lag in ORDER if f), tick, 0)

    @pl.when(last)
    def _():
        ltile[d] = jnp.full(ltile.shape[1:], 0.5 * jnp.sum(err_acc[...]), F32)
        for k in (2, 1, 3):
            send(ltile.at[d], ltile.at[d], l_sem.at[k], l_sem.at[n_model], peer(k), s).start()
        got(ltile.at[pl.ds(0, n_model - 1)], l_sem.at[n_model])
        ltile[n_model] = ltile[0] + ltile[1] + ltile[2] + ltile[3]
        for k in (1, 2, 3):
            sent(ltile.at[0], l_sem.at[k])

    @pl.when(jnp.logical_not(last))
    def _():
        got(ltile.at[n_model], chain_sem.at[0])

    for b in range(UNIT):
        sums_sent(0, b)
    peers = (1, 2, 3)
    for k in peers:
        sent(outs.at[0], o_sem.at[0, k])

    @pl.when(jnp.logical_not(last))
    def _():
        sent(outs.at[0], o_sem.at[0, 0])

    @pl.when(jnp.logical_not(first))
    def _():
        chain = send(ltile.at[n_model], ltile.at[n_model], chain_sem.at[1], chain_sem.at[0], d, down)
        chain.start()
        for b in range(UNIT):
            sums_sent(1, b)
        for k in (0, *peers):
            sent(outs.at[1], o_sem.at[1, k])
        chain.wait_send()

    loss_ref[0] = jnp.sum(ltile[n_model, 0:1, 0:1]) * scale
    for which in (0, 1):
        for j in range(hidden // tile):
            saved(which, j).wait()


def run_group(n_stage, tokens, x, t, w1, w2):
    num, n_model, rows, width = x.shape
    hidden = w1.shape[1]
    half = width // 2
    any_spec = pl.BlockSpec(memory_space=pl.ANY)
    vmem = pltpu.VMEM
    dma = pltpu.SemaphoreType.DMA
    flops = 12 * num * tokens * width * hidden
    return pl.pallas_call(
        functools.partial(kernel, n_stage),
        out_shape=(
            jax.ShapeDtypeStruct(w1.shape, F32),
            jax.ShapeDtypeStruct(w2.shape, F32),
            jax.ShapeDtypeStruct((1,), F32),
        ),
        in_specs=[any_spec] * 4,
        out_specs=(any_spec, any_spec, pl.BlockSpec(memory_space=pltpu.SMEM)),
        scratch_shapes=[
            vmem(w1.shape, BF16),
            vmem(w2.shape, BF16),
            vmem(w1.shape[::-1], BF16),
            vmem(w2.shape[::-1], BF16),
            vmem(w1.shape, F32),
            vmem(w2.shape, F32),
            vmem(x.shape, BF16),
            vmem((num // UNIT, UNIT * tokens, hidden), BF16),
            vmem(x.shape, BF16),
            vmem((UNIT * tokens, hidden), BF16),
            vmem((UNIT * tokens, hidden), BF16),
            vmem((2, 2, UNIT, n_model, rows, half), F32),
            vmem((2, SLOTS, 6, rows, half), F32),
            vmem((2, num, rows, width), BF16),
            vmem((rows, width), F32),
            vmem((n_model + 1, 8, 128), F32),
            dma((5,)),
            dma((2, num)),
            dma((2, SLOTS, 6)),
            dma((2, UNIT, 6)),
            dma((2, n_model)),
            dma((n_model + 1,)),
            dma((2,)),
            dma((2, 3)),
        ],
        compiler_params=pltpu.CompilerParams(
            collective_id=0, has_side_effects=True, vmem_limit_bytes=67043328
        ),
        cost_estimate=pl.CostEstimate(flops=flops, bytes_accessed=60 * width * hidden // 4, transcendentals=0),
        name="pipeline_step",
    )(x, t, w1, w2)


def solution(mesh):
    n_stage = mesh.shape["stage"]
    n_model = mesh.shape["model"]

    def stage_step(inputs, targets, w_in, w_out):
        width = inputs.shape[-1]
        total = inputs.shape[0] * inputs.shape[1]
        num = total // TOKENS
        shape = (num, n_model, TOKENS // n_model, width)
        dw1, dw2, loss = run_group(
            n_stage, TOKENS, inputs.reshape(shape), targets.reshape(shape), w_in[0, 0], w_out[0, 0])
        return dw1[None, None], dw2[None, None], loss

    return jax.shard_map(
        stage_step,
        mesh=mesh,
        in_specs=(P("data", None, None), P("data", None, None), P("stage", None, None, "model"), P("stage", None, "model", None)),
        out_specs=(P(("data", "stage"), None, None, "model"), P(("data", "stage"), None, "model", None), P("data")),
        check_vma=False,
    )
```

```python
import functools

import jax
import jax.numpy as jnp
from jax import lax
from jax.experimental import pallas as pl
from jax.experimental.pallas import tpu as pltpu
from jax.sharding import PartitionSpec as P

GELU_COEF = 0.7978845608028654
CUBIC_COEF = 0.044715
MESH = pl.DeviceIdType.MESH
F32 = jnp.float32
BF16 = jnp.bfloat16

TOKENS = 64
UNIT = 2
RING = 8
SLOTS = 2 * UNIT
AHEAD = (22, 19, 16, 13, 10, 7, 4, 1)
ORDER = (("A", 0, 0), ("T", 0, 0), ("E5", 1, 1), ("E4", 0, 0), ("A", 1, 0), ("G2", 1, 0), ("E5", 0, 0), ("G1", 1, 0), ("E4", 1, 0))
TN = (((0,), (0,)), ((), ()))


def dot(a, b, dims=(((1,), (0,)), ((), ()))):
    return lax.dot_general(a, b, dims, preferred_element_type=F32)


def kernel(n_stage, x_hbm, t_hbm, w1_hbm, w2_hbm, dw1, dw2, loss_ref,
           w1, w2, w1t, w2t, xs, us, es, ab, gb, ps, rs, outs, back, err_acc, ltile,
           load_sem, in_sem, r_sem, p_sem, o_sem, back_sem, l_sem, chain_sem):
    n_model = 4
    num, _, rows, width = xs.shape
    tokens = n_model * rows
    hidden = w1.shape[1]
    half = width // 2
    tile = min(512, hidden)
    scale = 1.0 / (num * tokens * width)
    s = lax.axis_index("stage")
    d = lax.axis_index("model")
    right = lax.rem(d + 1, n_model)
    left = lax.rem(d + 3, n_model)
    far = lax.rem(d + 2, n_model)
    first = s == 0
    last = s == n_stage - 1
    up = lax.rem(s + 1, n_stage)
    down = lax.rem(s + n_stage - 1, n_stage)
    ahead = jnp.int32(0)
    for k in range(n_stage):
        ahead = jnp.where(s == k, AHEAD[len(AHEAD) - n_stage + k], ahead)
    acts = (xs, es)

    def peer(k):
        return lax.rem(d + k, n_model)

    def send(src, dst, ssem, rsem, model, stage):
        return pltpu.make_async_remote_copy(
            src_ref=src, dst_ref=dst, send_sem=ssem, recv_sem=rsem,
            device_id={"model": model, "stage": stage}, device_id_type=MESH)

    def got(ref, sem):
        send(ref, ref, sem, sem, right, s).wait_recv()

    def sent(ref, sem):
        send(ref, ref, sem, sem, right, s).wait_send()

    units = num // UNIT
    tgt = outs
    load_w1 = pltpu.make_async_copy(w1_hbm, w1, load_sem.at[0])
    load_w2 = pltpu.make_async_copy(w2_hbm, w2, load_sem.at[1])
    load_x0 = pltpu.make_async_copy(x_hbm.at[pl.ds(0, UNIT)], xs.at[pl.ds(0, UNIT)], load_sem.at[2])
    load_x1 = pltpu.make_async_copy(
        x_hbm.at[pl.ds(UNIT, num - UNIT)], xs.at[pl.ds(UNIT, num - UNIT)], load_sem.at[3])
    load_t = pltpu.make_async_copy(t_hbm.at[:, d], tgt, load_sem.at[4])

    @pl.when(first)
    def _():
        load_x0.start()

    load_w1.start()
    load_w2.start()

    @pl.when(first)
    def _():
        load_x1.start()

    @pl.when(last)
    def _():
        load_t.start()

    barrier = pltpu.get_barrier_semaphore()
    for k in range(1, n_model):
        pl.semaphore_signal(barrier, inc=1, device_id={"model": peer(k), "stage": s}, device_id_type=MESH)
    for k in range(n_model):
        pl.semaphore_signal(barrier, inc=1, device_id={"model": peer(k), "stage": up}, device_id_type=MESH)
        pl.semaphore_signal(barrier, inc=1, device_id={"model": peer(k), "stage": down}, device_id_type=MESH)

    def zero(i, c):
        r = pl.ds(pl.multiple_of(i * 64, 64), 64)
        dw1[r, :] = jnp.zeros((64, dw1.shape[1]), F32)
        return c

    lax.fori_loop(0, dw1.shape[0] // 64, zero, 0)

    def zero2(i, c):
        r = pl.ds(pl.multiple_of(i * 64, 64), 64)
        dw2[r, :] = jnp.zeros((64, dw2.shape[1]), F32)
        return c

    lax.fori_loop(0, dw2.shape[0] // 64, zero2, 0)
    err_acc[...] = jnp.zeros_like(err_acc)
    pl.semaphore_wait(barrier, 3 * n_model - 1)

    pieces = hidden // 128
    assert width == hidden
    lazy = ahead > pieces

    def transpose(c):
        r = pl.ds(pl.multiple_of(c * 128, 128), 128)
        w2t[:, r] = w2[r, :].T
        w1t[:, r] = w1[r, :].T

    @pl.when(jnp.logical_not(lazy))
    def _():
        load_w1.wait()
        load_w2.wait()

        def piece(c, carry):
            transpose(c)
            return carry

        lax.fori_loop(0, pieces, piece, 0)

    @pl.when(last)
    def _():
        load_t.wait()

    def part(f, i, k):
        h, o, dev = ((0, far, right), (1, far, left), (1, right, right), (0, left, left), (0, right, right), (1, left, left))[k]
        b = lax.rem(i, UNIT)
        slot = lax.rem(i, SLOTS)
        return send(ps.at[f, h, b, o], rs.at[f, slot, k], p_sem.at[f, b, k], r_sem.at[f, slot, k], dev, s)

    def sums_sent(f, b):
        for k in range(6):
            sent(ps.at[0, 0, 0, 0], p_sem.at[f, b, k])

    def products(f, u, mat, weight):
        steps = [u * UNIT + k for k in range(UNIT)]

        @pl.when(u >= 1)
        def _():
            for k in range(UNIT):
                sums_sent(f, k)

        for h, kinds in ((0, (0,)), (1, (1, 2, 3))):
            ps[f, h] = weight(mat, h).reshape(UNIT, n_model, rows, half)
            for k in kinds:
                for i in steps:
                    part(f, i, k).start()

    def relay_sums(f, i):
        b = lax.rem(i, UNIT)
        slot = lax.rem(i, SLOTS)
        got(rs.at[f, slot, 0], r_sem.at[f, slot, 0])
        ps[f, 0, b, right] += rs[f, slot, 0]
        part(f, i, 4).start()
        got(rs.at[f, slot, 1], r_sem.at[f, slot, 1])
        ps[f, 1, b, left] += rs[f, slot, 1]
        part(f, i, 5).start()

    def final_sums(f, i):
        b = lax.rem(i, UNIT)
        slot = lax.rem(i, SLOTS)
        for k in (2, 3, 4, 5):
            got(rs.at[f, slot, k], r_sem.at[f, slot, k])
        base = acts[f][i, d]
        h0 = base[:, :half].astype(F32) + (ps[f, 0, b, d] + rs[f, slot, 4] + rs[f, slot, 3])
        h1 = base[:, half:].astype(F32) + (ps[f, 1, b, d] + rs[f, slot, 2] + rs[f, slot, 5])
        return h0.astype(BF16), h1.astype(BF16)

    def spread(f, i, src, stage, here):
        dst = acts[f].at[i, d]
        for k in (2, 1, 3) if here else (2, 1, 3, 0):
            send(src, dst, o_sem.at[k], in_sem.at[f, i], peer(k), stage).start()

    def arrived(f, i):
        if f:
            @pl.when(last)
            def _():
                got(es.at[i, pl.ds(0, n_model - 1)], in_sem.at[f, i])

            @pl.when(jnp.logical_not(last))
            def _():
                got(es.at[i], in_sem.at[f, i])
        else:
            got(xs.at[i], in_sem.at[f, i])

    def unit_rows(ref, u):
        return ref[pl.ds(u * UNIT, UNIT)].reshape(UNIT * tokens, width)

    def fwd(u):
        @pl.when(jnp.logical_not(first))
        def _():
            for k in range(UNIT):
                arrived(0, u * UNIT + k)

        @pl.when(jnp.logical_and(first, u <= 1))
        def _():
            @pl.when(u == 0)
            def _():
                load_x0.wait()

            @pl.when(u == 1)
            def _():
                load_x1.wait()

        start = jnp.logical_and(lazy, u == 0)

        @pl.when(start)
        def _():
            load_w1.wait()

        xm = unit_rows(xs, u)
        for j in range(hidden // tile):
            cols = slice(j * tile, (j + 1) * tile)
            pre = dot(xm, w1[:, cols]).astype(BF16)
            us[u, :, cols] = pre
            uf = pre.astype(F32)
            tau = jnp.tanh(GELU_COEF * (uf + CUBIC_COEF * uf * uf * uf))
            ab[:, cols] = (0.5 * uf * (1.0 + tau)).astype(BF16)

        @pl.when(start)
        def _():
            load_w2.wait()

        products(0, u, ab[...], lambda m, h: dot(m, w2[:, h * half:(h + 1) * half]))

    def fwd_out(i):
        ha, hb = final_sums(0, i)

        @pl.when(jnp.logical_not(last))
        def _():
            outs[i, :, :half] = ha
            outs[i, :, half:] = hb
            spread(0, i, outs.at[i], up, False)

        @pl.when(last)
        def _():
            for h, v in ((0, ha), (1, hb)):
                cols = slice(h * half, (h + 1) * half)
                err = v.astype(F32) - tgt[i, :, cols].astype(F32)
                es[i, d, :, cols] = (err * scale).astype(BF16)
                err_acc[:, cols] += err * err
            spread(1, i, es.at[i, d], s, True)

    def bwd_out(i):
        ha, hb = final_sums(1, i)
        slot = lax.rem(i, RING)

        @pl.when(i >= RING)
        def _():
            sent(back.at[pl.ds(0, n_model)], back_sem.at[slot])

        back[slot, :, :half] = ha
        back[slot, :, half:] = hb
        for k in (2, 1, 3, 0):
            send(back.at[slot], es.at[i, d], back_sem.at[slot], in_sem.at[1, i], peer(k), down).start()

    def grad_out(u):
        em = unit_rows(es, u)
        for j in range(hidden // tile):
            r = slice(j * tile, (j + 1) * tile)
            dw2[r, :] += dot(ab[:, r], em, TN)

    def grad_in(u):
        gm = gb[...]
        for j in range(width // tile):
            r = slice(j * tile, (j + 1) * tile)
            xt = xs[pl.ds(u * UNIT, UNIT), :, :, r].reshape(UNIT * tokens, tile)
            dw1[r, :] += dot(xt, gm, TN)

    def bwd(u):
        for k in range(UNIT):
            arrived(1, u * UNIT + k)
        em = unit_rows(es, u)
        for j in range(hidden // tile):
            cols = slice(j * tile, (j + 1) * tile)
            q = dot(em, w2t[:, cols]).astype(BF16).astype(F32)
            uf = us[u, :, cols].astype(F32)
            sq = uf * uf
            tau = jnp.tanh(GELU_COEF * (uf + CUBIC_COEF * uf * sq))
            slope = 0.5 * (1.0 + tau) + 0.5 * uf * (1.0 - tau * tau) * GELU_COEF * (1.0 + 3.0 * CUBIC_COEF * sq)
            gb[:, cols] = (slope * q).astype(BF16)
            ab[:, cols] = (0.5 * uf * (1.0 + tau)).astype(BF16)

        @pl.when(jnp.logical_not(first))
        def _():
            products(1, u, gb[...], lambda m, h: dot(m, w1t[:, h * half:(h + 1) * half]))

    def op(name, f, lag, tick):
        u = tick - lag - (ahead if f else 0)
        live = jnp.logical_and(u >= 0, u < units)
        if name == "A":
            run = bwd if f else fwd
        elif name == "T":
            run = lambda u: transpose(u - 1)
            live = jnp.logical_and(lazy, jnp.logical_and(u >= 1, u <= pieces))
        elif name == "G2":
            run = grad_out
        elif name == "G1":
            run = grad_in
        else:
            step = {
                "E4": functools.partial(relay_sums, f),
                "E5": bwd_out if f else fwd_out,
            }[name]

            def each(k, c):
                step(u * UNIT + k)
                return c

            def run(u):
                lax.fori_loop(0, UNIT, each, 0)

        if f and name in ("E4", "E5"):
            live = jnp.logical_and(live, jnp.logical_not(first))

        @pl.when(live)
        def _():
            run(u)

    def tick(t, c):
        for name, f, lag in ORDER:
            op(name, f, lag, t)
        return c

    begin = min(lag for _, _, lag in ORDER)
    lax.fori_loop(begin, units + ahead + max(lag for _, f, lag in ORDER if f), tick, 0)

    @pl.when(last)
    def _():
        ltile[d] = jnp.full(ltile.shape[1:], 0.5 * jnp.sum(err_acc[...]), F32)
        for k in (2, 1, 3):
            send(ltile.at[d], ltile.at[d], l_sem.at[k], l_sem.at[n_model], peer(k), s).start()
        got(ltile.at[pl.ds(0, n_model - 1)], l_sem.at[n_model])
        ltile[n_model] = ltile[0] + ltile[1] + ltile[2] + ltile[3]
        for k in (1, 2, 3):
            sent(ltile.at[0], l_sem.at[k])

    @pl.when(jnp.logical_not(last))
    def _():
        got(ltile.at[n_model], chain_sem.at[0])

    for b in range(UNIT):
        sums_sent(0, b)
    peers = (1, 2, 3)
    for k in peers:
        sent(outs, o_sem.at[k])

    @pl.when(jnp.logical_not(last))
    def _():
        sent(outs, o_sem.at[0])

    @pl.when(jnp.logical_not(first))
    def _():
        chain = send(ltile.at[n_model], ltile.at[n_model], chain_sem.at[1], chain_sem.at[0], d, down)
        chain.start()
        for b in range(UNIT):
            sums_sent(1, b)
        for slot in range(RING):
            sent(back.at[pl.ds(0, n_model)], back_sem.at[slot])
        chain.wait_send()

    loss_ref[0] = jnp.sum(ltile[n_model, 0:1, 0:1]) * scale


def run_group(n_stage, tokens, x, t, w1, w2):
    num, n_model, rows, width = x.shape
    hidden = w1.shape[1]
    half = width // 2
    any_spec = pl.BlockSpec(memory_space=pl.ANY)
    vmem = pltpu.VMEM
    dma = pltpu.SemaphoreType.DMA
    flops = 12 * num * tokens * width * hidden
    return pl.pallas_call(
        functools.partial(kernel, n_stage),
        out_shape=(
            vmem(w1.shape, F32),
            vmem(w2.shape, F32),
            jax.ShapeDtypeStruct((1,), F32),
        ),
        in_specs=[any_spec] * 4,
        out_specs=(pl.BlockSpec(memory_space=vmem), pl.BlockSpec(memory_space=vmem), pl.BlockSpec(memory_space=pltpu.SMEM)),
        scratch_shapes=[
            vmem(w1.shape, BF16),
            vmem(w2.shape, BF16),
            vmem(w1.shape[::-1], BF16),
            vmem(w2.shape[::-1], BF16),
            vmem(x.shape, BF16),
            vmem((num // UNIT, UNIT * tokens, hidden), BF16),
            vmem(x.shape, BF16),
            vmem((UNIT * tokens, hidden), BF16),
            vmem((UNIT * tokens, hidden), BF16),
            vmem((2, 2, UNIT, n_model, rows, half), F32),
            vmem((2, SLOTS, 6, rows, half), F32),
            vmem((num, rows, width), BF16),
            vmem((RING, rows, width), BF16),
            vmem((rows, width), F32),
            vmem((n_model + 1, 8, 128), F32),
            dma((5,)),
            dma((2, num)),
            dma((2, SLOTS, 6)),
            dma((2, UNIT, 6)),
            dma((n_model,)),
            dma((RING,)),
            dma((n_model + 1,)),
            dma((2,)),
        ],
        compiler_params=pltpu.CompilerParams(
            collective_id=0, has_side_effects=True, vmem_limit_bytes=48000000
        ),
        cost_estimate=pl.CostEstimate(flops=flops, bytes_accessed=60 * width * hidden // 4, transcendentals=0),
        name="pipeline_step",
    )(x, t, w1, w2)


def solution(mesh):
    n_stage = mesh.shape["stage"]
    n_model = mesh.shape["model"]

    def stage_step(inputs, targets, w_in, w_out):
        width = inputs.shape[-1]
        total = inputs.shape[0] * inputs.shape[1]
        num = total // TOKENS
        shape = (num, n_model, TOKENS // n_model, width)
        dw1, dw2, loss = run_group(
            n_stage, TOKENS, inputs.reshape(shape), targets.reshape(shape), w_in[0, 0], w_out[0, 0])
        return dw1[None, None], dw2[None, None], loss

    return jax.shard_map(
        stage_step,
        mesh=mesh,
        in_specs=(P("data", None, None), P("data", None, None), P("stage", None, None, "model"), P("stage", None, "model", None)),
        out_specs=(P(("data", "stage"), None, None, "model"), P(("data", "stage"), None, "model", None), P("data")),
        check_vma=False,
    )
```
